32 devices in a mesh: section: 2 (over x), tensor: 2 (over y), expert: 8 (over z, core).
Axes of the slice: x: 2, y: 2, z: 4, core: 2. Of those that a mesh axis runs over, the one named last changes fastest.
Arguments:
- saved_inputs: bfloat16 [2, 2, 512, 2048], P('section', None, 'expert', 'tensor'), may hold values from -64 to 64
- cot_in: bfloat16 [2, 512, 2048], P('section', 'expert', 'tensor'), may hold values from -6 to 6
- loss_grad: bfloat16 [512, 2048], P('expert', 'tensor'), may hold values from -6 to 6
- expert_ids: int32 [2, 2, 512, 2], P('section', None, 'expert'), may hold values from 0 to 3, all different within a row; in each aligned block of 64 rows (0 to 63, 64 to 127, ..., all dimensions but the last counted through in order) at most 48 rows name the same one
- route_weights: float32 [2, 2, 512, 2], P('section', None, 'expert'), may hold values from 0.05 to 0.5
- norm_gain: float32 [2, 2048], P('section', 'tensor'), may hold values from 0.12 to 8
- w_gate: bfloat16 [2, 8, 2048, 384], P('section', 'expert', 'tensor'), may hold values from -0.125 to 0.125
- w_up: bfloat16 [2, 8, 2048, 384], P('section', 'expert', 'tensor'), may hold values from -0.125 to 0.125
- w_down: bfloat16 [2, 8, 384, 2048], P('section', 'expert', None, 'tensor'), may hold values from -0.21875 to 0.21875
Outputs:
- input_grads: bfloat16 [2, 2, 512, 2048], P('section', None, 'expert', 'tensor')
The draws below stay inside these ranges and needn't reach their ends.
Inputs may be any that keep to these rules, and one draw needn't show every extreme that they name: `expert_ids`: each row names 2 different experts. Within each aligned block of 64 rows (the rows of one device in one micro-batch of one layer) no expert is named by more than 48 rows, and in some blocks one expert is named by exactly 48.
All inputs are finite; a program needn't handle non-finite values.
Results may differ from the reference program's by a relative error of at most 0.028.
Values may be sent and summed in bfloat16 or wider, within the bound.
A program may use at most 64 MiB of HBM per device.

```python
import math
import jax
import jax.numpy as jnp
import numpy as np
from jax import lax

D = 2048
FF = 768
TOK_MB = 64
LAYERS = 2
EXPERTS = 4
TOP = 2
CAP = 48
TOKENS = 512
N_TENSOR = 2
N_EXPERT = 8


def draw_saved_inputs(key, part):
    key_base, key_cols, key_rows = jax.random.split(key, 3)
    ramp = 3.0 ** (jnp.arange(D, dtype=jnp.float32) / D)
    columns = ramp * 10.0 ** (0.5 * jax.random.uniform(key_cols, (D,), jnp.float32))
    row_scale = 10.0 ** (jax.random.uniform(key_rows, (LAYERS, 2, TOKENS, 1), jnp.float32) - 0.5)
    base = jnp.clip(jax.random.normal(key_base, (LAYERS, 2, TOKENS, D), jnp.float32), -6.0, 6.0)
    return (base * columns * row_scale / 3.0).astype(jnp.bfloat16)


def draw_norm_gain(key, part):
    key_rough = jax.random.fold_in(key, 17)
    place = jnp.arange(D, dtype=jnp.float32) / D
    ramp = 0.25 * 16.0 ** place
    rough = 10.0 ** (0.3 * jax.random.uniform(key_rough, (LAYERS, D), jnp.float32) - 0.15)
    return (ramp[None, :] * rough).astype(jnp.float32)


def block_scale(stream_key, dims, cuts, smallest, top_value):
    def one(dim, blocks):
        steps = jax.random.uniform(jax.random.fold_in(jax.random.fold_in(stream_key, 6), dim), (blocks,), jnp.float32, smallest / len(cuts), top_value / len(cuts))
        return jnp.repeat(jnp.exp(steps), dims[dim] // blocks).reshape((-1,) + (1,) * (len(dims) - dim - 1))

    loudness = one(*cuts[0])
    for cut in cuts[1:]:
        loudness = loudness * one(*cut)
    return loudness


def routed_block(key, own, number, rows, count, top, reach, lean):
    sequence = jax.random.permutation(key, count)
    packed, usual = shares(count, rows * top, reach, lean, True), shares(count, rows * top, reach, lean, False)
    places = jnp.arange(count)

    def named(tallies, rotation):
        used = int((tallies > 0).sum())
        fixed = max(1, used // 4)
        shifted = fixed + (places - fixed + rotation * (used - fixed)) % max(1, count - fixed)
        return jnp.zeros((count,), jnp.int32).at[sequence[jnp.where(places < fixed, places, shifted)]].set(jnp.asarray(tallies, jnp.int32))

    tallies = jnp.where(number % 4 == 0, named(packed, number // 4), named(usual, number - number // 4 - 1))
    mixed = jax.random.permutation(jax.random.fold_in(own, 3), count)
    donor, taker = mixed[0:count // 2 * 2:2], mixed[1:count // 2 * 2:2]
    slack = jnp.minimum(tallies[donor] - 1, reach - tallies[taker]) // 2
    slack = jnp.where((donor == sequence[0]) | (taker == sequence[0]) | (tallies[taker] == 0), 0, jnp.maximum(slack, 0))
    shifted = jax.random.randint(jax.random.fold_in(own, 4), (count // 2,), 0, 1 << 20) % (slack + 1)
    tallies = tallies.at[donor].add(-shifted).at[taker].add(shifted)
    members = jnp.searchsorted(jnp.cumsum(tallies), jnp.arange(rows * top), side="right").astype(jnp.int32)
    listing = members.reshape(top, rows).T
    listing = listing[jax.random.permutation(jax.random.fold_in(own, 1), rows)]
    rotation = jax.random.randint(jax.random.fold_in(own, 2), (rows, 1), 0, top)
    return jnp.take_along_axis(listing, (jnp.arange(top)[None, :] + rotation) % top, axis=1)


def shares(amount, total, bound, lean, full):
    loads = [(1 << 20) // math.isqrt(grade ** lean) + 1 for grade in range(1, amount + 1)]
    largest = bound if full else min(bound, max(-(-total // amount), total * loads[0] // sum(loads)))
    least = 1 if total - largest >= amount - 1 else 0
    holding, rest = [largest] + [least] * (amount - 1), total - largest - least * (amount - 1)
    while rest > 0:
        movable = [i for i in range(1, amount) if holding[i] < largest] or [i for i in range(1, amount) if holding[i] < bound]
        whole, remaining = sum([loads[i] for i in movable]), rest
        for i in movable:
            more = min(bound - holding[i], max(1, remaining * loads[i] // whole), rest)
            holding[i] = holding[i] + more
            rest = rest - more
    return np.array(holding)


def bell_draw(stream_key, shape, width, bound, cuts=(), kind=jnp.bfloat16):
    drawn = jax.random.normal(stream_key, shape, jnp.float32) * width
    if len(cuts) > 0:
        drawn = block_scale(stream_key, shape, cuts, -0.22, 0.18) * drawn
    return jnp.clip(drawn, min=-bound, max=bound).astype(kind)


def setup_inputs(seed: int = 0) -> dict:
    key_of = jax.random.split(jax.random.key(seed), 10)
    saved_inputs = draw_saved_inputs(jax.random.fold_in(key_of[9], 71), 0)
    cot_in = bell_draw(key_of[1], (LAYERS, TOKENS, D), 1.0, 6.0, ((0, 2), (1, 8), (2, 2)))
    loss_grad = bell_draw(key_of[2], (TOKENS, D), 1.0, 6.0, ((0, 8), (1, 2)))
    expert_ids_keys = jax.random.split(jax.random.fold_in(key_of[3], 1), LAYERS * 2 * TOKENS // TOK_MB)
    expert_ids_turns = jax.random.permutation(jax.random.fold_in(key_of[3], 3), LAYERS * 2 * TOKENS // TOK_MB)
    expert_ids = jax.vmap(lambda own, number: routed_block(jax.random.fold_in(key_of[3], 2), own, number, TOK_MB, EXPERTS, TOP, CAP, 2))(expert_ids_keys, expert_ids_turns).reshape((LAYERS, 2, TOKENS, TOP))
    route_weights = jnp.clip(jnp.exp(math.log(0.5) - 2.3025851 * jax.random.uniform(key_of[4], (LAYERS, 2, TOKENS, TOP), jnp.float32) ** block_scale(key_of[4], (LAYERS, 2, TOKENS, TOP), ((0, 2), (2, 8)), -0.2, 0.2)), 0.05, 0.5)
    norm_gain = draw_norm_gain(jax.random.fold_in(key_of[9], 71), 0)
    w_gate = bell_draw(key_of[6], (LAYERS, 2 * EXPERTS, D, FF // 2), D ** -0.5, 0.125, ((0, 2), (1, 8), (2, 2)))
    w_up = bell_draw(key_of[7], (LAYERS, 2 * EXPERTS, D, FF // 2), D ** -0.5, 0.125, ((0, 2), (1, 8), (2, 2)))
    w_down = bell_draw(key_of[8], (LAYERS, 2 * EXPERTS, FF // 2, D), FF ** -0.5, 0.21875, ((0, 2), (1, 8), (3, 2)))
    return {"saved_inputs": saved_inputs, "cot_in": cot_in, "loss_grad": loss_grad, "expert_ids": expert_ids, "route_weights": route_weights, "norm_gain": norm_gain, "w_gate": w_gate, "w_up": w_up, "w_down": w_down}


epsilon = 1e-06

def silu_grad(values):
    sigma = jax.nn.sigmoid(values)
    return sigma * (1.0 + values * (1.0 - sigma))

def product(left, right):
    return jnp.dot(left.astype(jnp.float32), right.astype(jnp.float32), precision=lax.Precision.HIGHEST)

def rounded(values):
    return lax.optimization_barrier(values.astype(jnp.bfloat16)).astype(jnp.float32)

def slot_tables(route_ids, weights):
    blocks = route_ids.reshape(N_EXPERT, TOK_MB * TOP)
    onehot = (blocks[:, :, None] == jnp.arange(EXPERTS, dtype=jnp.int32)[None, None, :]).astype(jnp.int32)
    before = jnp.cumsum(onehot, axis=1) - onehot
    position = lax.optimization_barrier(jnp.sum(before * onehot, axis=2))
    source = jnp.arange(N_EXPERT, dtype=jnp.int32)[:, None]
    flat_slot = (blocks * (N_EXPERT * CAP) + source * CAP + position).reshape(-1).astype(jnp.int32)
    token_index = jnp.repeat(jnp.arange(TOKENS, dtype=jnp.int32), TOP)
    slot_total = EXPERTS * N_EXPERT * CAP
    token_of = jnp.full((slot_total,), TOKENS, jnp.int32).at[flat_slot].set(token_index)
    weight_of = jnp.zeros((slot_total,), jnp.float32).at[flat_slot].set(weights.reshape(-1))
    return (token_of, weight_of)

def expert_back(operands):
    rows_in, rows_grad, gate_weights, up_weights, down_weights = operands
    group = D // N_TENSOR
    pieces = []
    for part_index in range(2):
        gate_sum = jnp.zeros((rows_in.shape[0], FF // 2), jnp.float32)
        up_sum = jnp.zeros((rows_in.shape[0], FF // 2), jnp.float32)
        hidden = jnp.zeros((rows_in.shape[0], FF // 2), jnp.float32)
        for rank_index in range(N_TENSOR):
            low = rank_index * group
            high = low + group
            gate_sum = gate_sum + rounded(product(rows_in[:, low:high], gate_weights[part_index, low:high]))
            up_sum = up_sum + rounded(product(rows_in[:, low:high], up_weights[part_index, low:high]))
            hidden = hidden + rounded(product(rows_grad[:, low:high], down_weights[part_index][:, low:high].T))
        grad_gate = (hidden * up_sum * silu_grad(gate_sum)).astype(jnp.bfloat16)
        grad_up = (hidden * jax.nn.silu(gate_sum)).astype(jnp.bfloat16)
        grad_piece = product(grad_gate, gate_weights[part_index].T) + product(grad_up, up_weights[part_index].T)
        pieces.append(grad_piece.astype(jnp.bfloat16))
    return jnp.stack(pieces)

def layer_back(inputs, incoming, route_ids, weights, gain_row, gate_weights, up_weights, down_weights):
    values = inputs.astype(jnp.float32)
    squares = lax.optimization_barrier(jnp.sum(values * values, axis=1, keepdims=True))
    root_mean = jnp.sqrt(squares / D + epsilon)
    normed = values / root_mean
    expert_input = (normed * gain_row[None, :]).astype(jnp.bfloat16)
    token_of, weight_of = slot_tables(route_ids, weights)
    padded_input = jnp.concatenate([expert_input, jnp.zeros((1, D), jnp.bfloat16)], axis=0)
    padded_grad = jnp.concatenate([incoming, jnp.zeros((1, D), jnp.bfloat16)], axis=0)
    rows_in = padded_input[token_of].reshape(EXPERTS, N_EXPERT * CAP, D)
    rows_grad = (weight_of[:, None] * padded_grad[token_of].astype(jnp.float32)).astype(jnp.bfloat16)
    rows_grad = rows_grad.reshape(EXPERTS, N_EXPERT * CAP, D)
    pieces = lax.map(expert_back, (rows_in, rows_grad, gate_weights.reshape(EXPERTS, 2, D, FF // 2), up_weights.reshape(EXPERTS, 2, D, FF // 2), down_weights.reshape(EXPERTS, 2, FF // 2, D)))
    summed = lax.optimization_barrier(jnp.sum(pieces.astype(jnp.float32), axis=1)).reshape(-1, D)
    cot_normed = jax.ops.segment_sum(summed, token_of, TOKENS + 1)[:TOKENS]
    scaled = gain_row[None, :] * cot_normed
    inner = lax.optimization_barrier(jnp.sum(normed * scaled, axis=1, keepdims=True))
    return (incoming.astype(jnp.float32) + (scaled - normed * (inner / D)) / root_mean).astype(jnp.bfloat16)

def reference(saved_inputs, cot_in, loss_grad, expert_ids, route_weights, norm_gain, w_gate, w_up, w_down):

    def first_layer(layer):
        return layer_back(saved_inputs[layer, 0], cot_in[layer], expert_ids[layer, 0], route_weights[layer, 0], norm_gain[layer], w_gate[layer], w_up[layer], w_down[layer])
    first_pass = lax.map(first_layer, jnp.arange(LAYERS, dtype=jnp.int32))
    following = jnp.concatenate([first_pass[1:], loss_grad[None]], axis=0)

    def second_layer(layer):
        return layer_back(saved_inputs[layer, 1], following[layer], expert_ids[layer, 1], route_weights[layer, 1], norm_gain[layer], w_gate[layer], w_up[layer], w_down[layer])
    second_pass = lax.map(second_layer, jnp.arange(LAYERS, dtype=jnp.int32))
    return jnp.stack([first_pass, second_pass], axis=1)
```

```python
import jax
import jax.numpy as jnp
from jax import lax
from jax.experimental import pallas as pl
from jax.experimental.pallas import tpu as pltpu
from jax.sharding import PartitionSpec as P

epsilon = 1e-06
MESH = pl.DeviceIdType.MESH
bf16 = jnp.bfloat16
f32 = jnp.float32


def contract_last(left, right):
    return lax.dot_general(left, right, (((1,), (1,)), ((), ())), preferred_element_type=f32)


def contract_first(left, right):
    return lax.dot_general(left, right, (((0,), (0,)), ((), ())), preferred_element_type=f32)


def dot(left, right):
    return jnp.dot(left, right, preferred_element_type=f32)


def make_kernel(sections, tensors, experts, capacity):

    def kernel(
        saved, cot_in, loss_grad, ids, weights, gain, wg_hbm, wu_hbm, wd_hbm, out,
        wgu, wd, w_sem, choose, picked, rows_out, rows, part_gu, part_h,
        gu_send, gu_recv, h_send, h_recv, grads, ret_send, ret_recv,
        sc_send, sc_recv, sq_send, sq_recv, sec_recv,
        w_s, w_r, d_s, d_r, y_s, y_r, r_s, r_r, v_s, v_r, q_s, q_r, c_s, c_r,
    ):
        s = lax.axis_index("section")
        t = lax.axis_index("tensor")
        x = lax.axis_index("expert")
        e, q = x // 2, x % 2
        tok = saved.shape[2]
        feat = saved.shape[3]
        top = ids.shape[2]
        hid = wd_hbm.shape[2]
        model = feat * tensors
        js = list(range(experts))

        loads = [
            pltpu.make_async_copy(wd_hbm.at[0, 0], wd.at[0:hid], w_sem.at[0]),
            pltpu.make_async_copy(wg_hbm.at[0, 0], wgu.at[:, 0:hid], w_sem.at[1]),
            pltpu.make_async_copy(wu_hbm.at[0, 0], wgu.at[:, 2 * hid : 3 * hid], w_sem.at[2]),
        ]
        for load in loads:
            load.start()

        def expert_at(j):
            other, bit = e, 1
            while bit < experts:
                if j & bit:
                    other = other + bit - 2 * bit * ((e // bit) % 2)
                bit *= 2
            return other

        lane_peer = lambda j: (s, t, 2 * expert_at(j) + q)
        partner = (s, t, 2 * e + 1 - q)
        y_peer = (s, 1 - t, x)

        barrier = pltpu.get_barrier_semaphore()
        greet = [lane_peer(j) for j in js[1:]] + [partner, y_peer]
        for device in greet:
            pl.semaphore_signal(barrier, inc=1, device_id=device, device_id_type=MESH)

        @pl.when(s > 0)
        def _():
            pl.semaphore_signal(barrier, inc=1, device_id=(s - 1, t, x), device_id_type=MESH)

        @pl.when(s < sections - 1)
        def _():
            pl.semaphore_signal(barrier, inc=1, device_id=(s + 1, t, x), device_id_type=MESH)

        def remote(src, dst, send, recv, device):
            return pltpu.make_async_remote_copy(
                src_ref=src, dst_ref=dst, send_sem=send, recv_sem=recv,
                device_id=device, device_id_type=MESH,
            )

        def weight_copy(i):
            ref = (
                (wd.at[0:hid], wd.at[hid : 2 * hid]),
                (wgu.at[:, 0:hid], wgu.at[:, hid : 2 * hid]),
                (wgu.at[:, 2 * hid : 3 * hid], wgu.at[:, 3 * hid : 4 * hid]),
            )[i]
            return remote(ref[0], ref[1], w_s.at[i], w_r.at[i], partner)

        def direct(m, k, j):
            return remote(
                rows_out.at[m, k, j], rows.at[m, k, j], d_s.at[m, k, j], d_r.at[m, k, j],
                lane_peer(j),
            )

        def exchange(m, k, i):
            lo, n = chunks[i]
            src, dst = ((gu_send, gu_recv), (h_send, h_recv))[k]
            return remote(
                src.at[m, lo : lo + n], dst.at[m, lo : lo + n], y_s.at[m, k, i], y_r.at[m, k, i],
                y_peer,
            )

        def give_back(m, j):
            return remote(
                ret_send.at[m, j], ret_recv.at[m, j], r_s.at[m, j], r_r.at[m, j], lane_peer(j)
            )

        def give_scalars(m, j):
            return remote(
                sc_send.at[m, j], sc_recv.at[m, j], v_s.at[m, j], v_r.at[m, j], lane_peer(j)
            )

        def squares_copy():
            return remote(sq_send, sq_recv, q_s, q_r, y_peer)

        def section_copy():
            return remote(out.at[0, 0], sec_recv, c_s, c_r, (s - 1, t, x))

        started = []

        def start(copy):
            copy.start()
            started.append(copy)

        quarter = max(1, experts // 4)
        chunks = [(0, 2 * quarter), (3 * quarter, quarter), (2 * quarter, quarter)]
        order = js[3 * quarter :] + js[1 : 2 * quarter] + js[2 * quarter : 3 * quarter]

        height = max(8, experts)
        lane = lax.broadcasted_iota(jnp.int32, (tok, 128), 1)
        row = lax.broadcasted_iota(jnp.int32, (height, tok), 0)
        named = jnp.full((height, tok), experts, jnp.int32)
        for j in js:
            named = jnp.where(row == j, expert_at(j), named)
        later = (
            lax.broadcasted_iota(jnp.int32, (tok, tok), 0)
            < lax.broadcasted_iota(jnp.int32, (tok, tok), 1)
        ).astype(f32).astype(bf16)
        slot = lax.broadcasted_iota(jnp.int32, (capacity, tok), 0).astype(f32)
        for m in range(2):
            hit = jnp.zeros((height, tok), f32)
            weight = jnp.zeros((height, tok), f32)
            for k in range(top):
                same = (ids[0, m, k : k + 1, :] == named).astype(f32)
                hit = hit + same
                weight = weight + same * weights[0, m, k : k + 1, :]
            position = dot(hit.astype(bf16), later)
            for j in js:
                chosen = (position[j : j + 1] == slot).astype(f32) * hit[j : j + 1]
                choose[m, j] = chosen.astype(bf16)
                picked[m, j] = jnp.broadcast_to(
                    jnp.sum(chosen * weight[j : j + 1], axis=1, keepdims=True), (capacity, 128)
                )
        square = []
        for m in range(2):
            values = saved[0, m].astype(f32)
            square.append(jnp.sum(values * values, axis=1, keepdims=True))
        sq_send[...] = jnp.where(lane < 64, square[0], square[1])

        def pack(m, k, value):
            packed = dot(choose[m].reshape(experts * capacity, tok), value)
            packed = packed.reshape(experts, capacity, feat)
            if k == 1:
                packed = packed * picked[m][:, :, :1]
            packed = packed.astype(bf16)
            rows[m, k, 0] = packed[0]
            rows_out[m, k, 1:] = packed[1:]

        for load in loads:
            load.wait()
        neighbours = (s > 0).astype(jnp.int32) + (s < sections - 1).astype(jnp.int32)
        pl.semaphore_wait(barrier, len(greet) + neighbours)

        start(squares_copy())
        pack(0, 1, cot_in[0])
        for j in order:
            start(direct(0, 1, j))
        for i in range(3):
            start(weight_copy(i))

        squares_copy().wait_recv()
        total = sq_send[...] + sq_recv[...]
        roots = [
            jnp.sqrt(total[:, 64 * m : 64 * m + 1] / model + epsilon) for m in range(2)
        ]

        def normed_of(m):
            return saved[0, m].astype(f32) / roots[m]

        def expert_input(m):
            return (normed_of(m) * gain[...]).astype(bf16)

        pack(0, 0, expert_input(0))
        for j in order:
            start(direct(0, 0, j))
        pack(1, 0, expert_input(1))

        @pl.when(s == 0)
        def _():
            for j in order:
                direct(1, 0, j).start()

        for i in range(3):
            weight_copy(i).wait_recv()

        def consume(m, k, i):
            lo, n = chunks[i]
            for j in range(max(1, lo), lo + n):
                direct(m, k, j).wait_recv()
            flat = rows[m, k, lo : lo + n].reshape(n * capacity, feat)
            if k == 0:
                done = dot(flat, wgu[...]).reshape(n, capacity, 4 * hid)
                part_gu[m, lo : lo + n] = done
                gu_send[m, lo : lo + n] = done.astype(bf16)
            else:
                done = contract_last(flat, wd[...]).reshape(n, capacity, 2 * hid)
                part_h[m, lo : lo + n] = done
                h_send[m, lo : lo + n] = done.astype(bf16)
            exchange(m, k, i).start()

        def produce(m, i):
            lo, n = chunks[i]
            exchange(m, 0, i).wait_recv()
            exchange(m, 1, i).wait_recv()
            ones = jnp.ones((8, 2 * hid), bf16)
            for j in range(lo, lo + n):
                both = part_gu[m, j] + gu_recv[m, j].astype(f32)
                hidden = part_h[m, j] + h_recv[m, j].astype(f32)
                gate, up = both[:, : 2 * hid], both[:, 2 * hid :]
                sigma = jax.nn.sigmoid(gate)
                grad_gate = hidden * up * (sigma * (1.0 + gate * (1.0 - sigma)))
                grad_up = hidden * (gate * sigma)
                grads[m, j, :, : 2 * hid] = grad_gate.astype(bf16)
                grads[m, j, :, 2 * hid :] = grad_up.astype(bf16)
                inner = (grad_gate * gate + grad_up * up).astype(bf16)
                scalars = contract_last(ones, inner)
                if j == 0:
                    sc_recv[m, j, :, :capacity] = scalars
                else:
                    sc_send[m, j, :, :capacity] = scalars
                    start(give_scalars(m, j))
            flat = grads[m, lo : lo + n].reshape(n * capacity, 4 * hid)
            done = contract_last(flat, wgu[...]).reshape(n, capacity, feat).astype(bf16)
            for j in range(lo, lo + n):
                if j == 0:
                    ret_recv[m, 0] = done[0]
                else:
                    ret_send[m, j] = done[j - lo]
                    start(give_back(m, j))

        def combine(m, incoming):
            for j in js[1:]:
                give_scalars(m, j).wait_recv()
            inner = jnp.zeros((tok, 8), f32)
            for j in js:
                inner = inner + lax.dot_general(
                    choose[m, j], sc_recv[m, j, :, :capacity].astype(bf16),
                    (((0,), (1,)), ((), ())), preferred_element_type=f32,
                )
            inner = inner[:, :1]
            for j in js[1:]:
                give_back(m, j).wait_recv()
            cot = contract_first(
                choose[m].reshape(experts * capacity, tok),
                ret_recv[m].reshape(experts * capacity, feat),
            )
            scaled = gain[...] * cot
            normed = normed_of(m)
            out[0, m] = (
                incoming + (scaled - normed * (inner / model)) / roots[m]
            ).astype(bf16)

        consume(0, 1, 1)
        consume(0, 1, 0)
        consume(0, 1, 2)
        consume(0, 0, 1)
        consume(0, 0, 0)
        consume(0, 0, 2)
        produce(0, 1)
        produce(0, 0)
        produce(0, 2)

        @pl.when(s == 0)
        def _():
            for i in (1, 0, 2):
                consume(1, 0, i)

        @pl.when(s > 0)
        def _():
            for j in order:
                direct(1, 0, j).start()

        @pl.when(s == sections - 1)
        def _():
            sec_recv[...] = loss_grad[...]
            pack(1, 1, sec_recv[...])
            for j in order:
                direct(1, 1, j).start()

        combine(0, cot_in[0].astype(f32))

        @pl.when(s > 0)
        def _():
            section_copy().start()
            for i in (1, 0, 2):
                consume(1, 0, i)

        @pl.when(s < sections - 1)
        def _():
            section_copy().wait_recv()
            pack(1, 1, sec_recv[...])
            for j in order:
                direct(1, 1, j).start()

        for i in (1, 0, 2):
            consume(1, 1, i)
        for i in (1, 0, 2):
            produce(1, i)
        combine(1, sec_recv[...].astype(f32))

        for copy in started:
            copy.wait_send()
        for j in js[1:]:
            for k in range(2):
                direct(1, k, j).wait_send()
        for m in range(2):
            for k in range(2):
                for i in range(3):
                    exchange(m, k, i).wait_send()

        @pl.when(s > 0)
        def _():
            section_copy().wait_send()

    return kernel


def solution(mesh):
    sections, tensors = mesh.shape["section"], mesh.shape["tensor"]
    experts = mesh.shape["expert"] // 2

    def local(saved, cot_in, loss_grad, ids, weights, gain, wg, wu, wd):
        tok, feat = saved.shape[2], saved.shape[3]
        hid = wg.shape[3]
        named = 3 * tok * ids.shape[3] // (2 * experts)
        cap = -(-named // 16) * 16
        vmem = pl.BlockSpec(memory_space=pltpu.VMEM)
        hbm = pl.BlockSpec(memory_space=pl.ANY)
        dma = pltpu.SemaphoreType.DMA
        scratch = [
            pltpu.VMEM((feat, 4 * hid), bf16), pltpu.VMEM((2 * hid, feat), bf16), dma((3,)),
            pltpu.VMEM((2, experts, cap, tok), bf16), pltpu.VMEM((2, experts, cap, 128), f32),
            pltpu.VMEM((2, 2, experts, cap, feat), bf16),
            pltpu.VMEM((2, 2, experts, cap, feat), bf16),
            pltpu.VMEM((2, experts, cap, 4 * hid), f32),
            pltpu.VMEM((2, experts, cap, 2 * hid), f32),
            pltpu.VMEM((2, experts, cap, 4 * hid), bf16),
            pltpu.VMEM((2, experts, cap, 4 * hid), bf16),
            pltpu.VMEM((2, experts, cap, 2 * hid), bf16),
            pltpu.VMEM((2, experts, cap, 2 * hid), bf16),
            pltpu.VMEM((2, experts, cap, 4 * hid), bf16),
            pltpu.VMEM((2, experts, cap, feat), bf16),
            pltpu.VMEM((2, experts, cap, feat), bf16),
            pltpu.VMEM((2, experts, 8, 128), f32), pltpu.VMEM((2, experts, 8, 128), f32),
            pltpu.VMEM((tok, 128), f32), pltpu.VMEM((tok, 128), f32),
            pltpu.VMEM((tok, feat), bf16),
        ]
        pair = [dma, dma]
        scratch += [dma((3,))] * 2 + [dma((2, 2, experts))] * 2 + [dma((2, 2, 3))] * 2
        scratch += [dma((2, experts))] * 4 + pair + pair
        return pl.pallas_call(
            make_kernel(sections, tensors, experts, cap),
            out_shape=jax.ShapeDtypeStruct((1, 2, tok, feat), bf16),
            in_specs=[vmem] * 6 + [hbm] * 3,
            out_specs=vmem,
            scratch_shapes=scratch,
            compiler_params=pltpu.CompilerParams(
                collective_id=0, has_side_effects=True, vmem_limit_bytes=62 * 1024 * 1024
            ),
            name="expert_back",
        )(
            saved, cot_in, loss_grad, ids.transpose(0, 1, 3, 2), weights.transpose(0, 1, 3, 2),
            gain, wg, wu, wd,
        )

    in_specs = (
        P("section", None, "expert", "tensor"),
        P("section", "expert", "tensor"),
        P("expert", "tensor"),
        P("section", None, "expert", None),
        P("section", None, "expert", None),
        P("section", "tensor"),
        P("section", "expert", "tensor", None),
        P("section", "expert", "tensor", None),
        P("section", "expert", None, "tensor"),
    )
    out_specs = P("section", None, "expert", "tensor")
    return jax.shard_map(local, mesh=mesh, in_specs=in_specs, out_specs=out_specs, check_vma=False)
```

```python
import jax
import jax.numpy as jnp
from jax import lax
from jax.experimental import pallas as pl
from jax.experimental.pallas import tpu as pltpu
from jax.sharding import PartitionSpec as P

epsilon = 1e-06
MESH = pl.DeviceIdType.MESH
bf16 = jnp.bfloat16
f32 = jnp.float32


def contract_last(left, right):
    return lax.dot_general(left, right, (((1,), (1,)), ((), ())), preferred_element_type=f32)


def contract_first(left, right):
    return lax.dot_general(left, right, (((0,), (0,)), ((), ())), preferred_element_type=f32)


def dot(left, right):
    return jnp.dot(left, right, preferred_element_type=f32)


def make_kernel(sections, tensors, experts, capacity):

    def kernel(
        saved, cot_in, loss_grad, ids, weights, gain, wg_hbm, wu_hbm, wd_hbm, out,
        wgu, wd, w_sem, choose, picked, rows_out, rows, part_gu, part_h, part_in,
        gu_send, gu_recv, h_send, h_recv, grads, ret_send, ret_recv,
        sc_send, sc_recv, sq_send, sq_recv, sec_recv,
        xin, full_recv, ids_far, weights_far, choose_far, picked_far,
        rows_up, ids_up, weights_up, choose_up, picked_up,
        rows_top, ids_top, weights_top, choose_top, picked_top,
        w_s, w_r, d_s, d_r, y_s, y_r, r_s, r_r, v_s, v_r, q_s, q_r, c_s, c_r,
        f_s, f_r, i_s, i_r, u_s, g_s, g_r, t_s, h_s, h_r,
    ):
        s = lax.axis_index("section")
        t = lax.axis_index("tensor")
        x = lax.axis_index("expert")
        e, q = x // 2, x % 2
        tok = saved.shape[2]
        feat = saved.shape[3]
        top = ids.shape[2]
        hid = wd_hbm.shape[2]
        model = feat * tensors
        js = list(range(experts))

        loads = [
            pltpu.make_async_copy(wd_hbm.at[0, 0], wd.at[0:hid], w_sem.at[0]),
            pltpu.make_async_copy(wg_hbm.at[0, 0], wgu.at[:, 0:hid], w_sem.at[1]),
            pltpu.make_async_copy(wu_hbm.at[0, 0], wgu.at[:, 2 * hid : 3 * hid], w_sem.at[2]),
        ]
        for load in loads:
            load.start()

        line = experts == 4
        relayed = ((False, True), (True, False)) if line else ((False, False), (False, False))
        side = e // 2
        inner = ((e + 1) // 2) % 2
        far_slot = 3 - inner

        def expert_at(j):
            if line and j >= 2:
                return 2 - side if j == 2 else 3 * (1 - side)
            other, bit = e, 1
            while bit < experts:
                if j & bit:
                    other = other + bit - 2 * bit * ((e // bit) % 2)
                bit *= 2
            return other

        lane_peer = lambda j: (s, t, 2 * expert_at(j) + q)
        partner = (s, t, 2 * e + 1 - q)
        y_peer = (s, 1 - t, x)

        barrier = pltpu.get_barrier_semaphore()
        greet = [lane_peer(j) for j in js[1:]] + [partner, y_peer]
        for device in greet:
            pl.semaphore_signal(barrier, inc=1, device_id=device, device_id_type=MESH)

        @pl.when(s > 0)
        def _():
            for j in js:
                below = (s - 1, t, 2 * expert_at(j) + q)
                pl.semaphore_signal(barrier, inc=1, device_id=below, device_id_type=MESH)

        @pl.when(s < sections - 1)
        def _():
            for j in js:
                above = (s + 1, t, 2 * expert_at(j) + q)
                pl.semaphore_signal(barrier, inc=1, device_id=above, device_id_type=MESH)

        def remote(src, dst, send, recv, device):
            return pltpu.make_async_remote_copy(
                src_ref=src, dst_ref=dst, send_sem=send, recv_sem=recv,
                device_id=device, device_id_type=MESH,
            )

        def weight_copy(i):
            ref = (
                (wd.at[0:hid], wd.at[hid : 2 * hid]),
                (wgu.at[:, 0:hid], wgu.at[:, hid : 2 * hid]),
                (wgu.at[:, 2 * hid : 3 * hid], wgu.at[:, 3 * hid : 4 * hid]),
            )[i]
            return remote(ref[0], ref[1], w_s.at[i], w_r.at[i], partner)

        def landing(j):
            return far_slot if line and j >= 2 else j

        def direct(m, k, j):
            return remote(
                rows_out.at[m, k, j], rows.at[m, k, landing(j)],
                d_s.at[m, k, j], d_r.at[m, k, landing(j)], lane_peer(j),
            )

        def passed_on(m, k):
            return remote(
                rows_out.at[m, k, 2], rows.at[m, k, 2], d_s.at[m, k, 2], d_r.at[m, k, 2],
                lane_peer(1),
            )

        def arrival(m, k, j):
            return remote(
                rows_out.at[m, k, j], rows.at[m, k, j], d_s.at[m, k, j], d_r.at[m, k, j],
                lane_peer(j),
            )

        def whole(m, k):
            src = xin.at[m] if k == 0 else (cot_in.at[0], sec_recv)[m]
            return remote(src, full_recv.at[m, k], f_s.at[m, k], f_r.at[m, k], lane_peer(2))

        def routes(i):
            src, dst = ((ids, ids_far), (weights, weights_far))[i]
            return remote(src, dst, i_s.at[i], i_r.at[i], lane_peer(2))

        def send_rows(m, k):
            if not relayed[m][k]:
                for j in js[1:] if line else order:
                    direct(m, k, j).start()
                return

            @pl.when(inner == 1)
            def _():
                whole(m, k).start()
                direct(m, k, 1).start()

            @pl.when(inner == 0)
            def _():
                for j in (1, 2, 3):
                    direct(m, k, j).start()

        def exchange(m, k, i):
            lo, n = chunks[i]
            src, dst = ((gu_send, gu_recv), (h_send, h_recv))[k]
            return remote(
                src.at[m, lo : lo + n], dst.at[m, lo : lo + n], y_s.at[m, k, i], y_r.at[m, k, i],
                y_peer,
            )

        def give_back(m, j):
            return remote(
                ret_send.at[m, j], ret_recv.at[m, landing(j)], r_s.at[m, j],
                r_r.at[m, landing(j)], lane_peer(j),
            )

        def given_back(m, j):
            return remote(
                ret_send.at[m, j], ret_recv.at[m, j], r_s.at[m, j], r_r.at[m, j], lane_peer(j)
            )

        def give_scalars(m, j):
            return remote(
                sc_send.at[m, j], sc_recv.at[m, landing(j)], v_s.at[m, j],
                v_r.at[m, landing(j)], lane_peer(j),
            )

        def given_scalars(m, j):
            return remote(
                sc_send.at[m, j], sc_recv.at[m, j], v_s.at[m, j], v_r.at[m, j], lane_peer(j)
            )

        def squares_copy():
            return remote(sq_send, sq_recv, q_s, q_r, y_peer)

        def section_copy():
            return remote(out.at[0, 0], sec_recv, c_s, c_r, (s - 1, t, x))

        def descend(j):
            return remote(
                rows_up.at[j], rows.at[1, 1, landing(j)], u_s.at[j], d_r.at[1, 1, landing(j)],
                (s - 1, t, 2 * expert_at(j) + q),
            )

        def ascend(j):
            return remote(
                rows_top.at[j], rows.at[1, 1, landing(j)], t_s.at[j], d_r.at[1, 1, landing(j)],
                (s + 1, t, 2 * expert_at(j) + q),
            )

        def routes_top(i):
            src, dst = ((ids, ids_top), (weights, weights_top))[i]
            return remote(src, dst, h_s.at[i], h_r.at[i], (s - 1, t, x))

        def routes_up(i):
            src, dst = ((ids, ids_up), (weights, weights_up))[i]
            return remote(src, dst, g_s.at[i], g_r.at[i], (s + 1, t, x))

        started = []

        def start(copy):
            copy.start()
            started.append(copy)

        quarter = max(1, experts // 4)
        near, far = js[1 : 2 * quarter], js[2 * quarter :]
        chunks = [(i * quarter, quarter) for i in range(experts // quarter)]
        order = js[3 * quarter :] + js[1 : 2 * quarter] + js[2 * quarter : 3 * quarter]

        lane = lax.broadcasted_iota(jnp.int32, (tok, 128), 1)
        later = (
            lax.broadcasted_iota(jnp.int32, (tok, tok), 0)
            < lax.broadcasted_iota(jnp.int32, (tok, tok), 1)
        ).astype(f32).astype(bf16)
        slot = lax.broadcasted_iota(jnp.int32, (capacity, tok), 0).astype(f32)

        def tables(ids, weights, count, choose, picked, batches=(0, 1)):
            height = max(8, count)
            row = lax.broadcasted_iota(jnp.int32, (height, tok), 0)
            named = jnp.full((height, tok), experts, jnp.int32)
            for j in range(count):
                named = jnp.where(row == j, expert_at(j), named)
            for m in batches:
                hit = jnp.zeros((height, tok), f32)
                weight = jnp.zeros((height, tok), f32)
                for k in range(top):
                    same = (ids[0, m, k : k + 1, :] == named).astype(f32)
                    hit = hit + same
                    weight = weight + same * weights[0, m, k : k + 1, :]
                position = dot(hit.astype(bf16), later)
                for j in range(count):
                    chosen = (position[j : j + 1] == slot).astype(f32) * hit[j : j + 1]
                    choose[m, j] = chosen.astype(bf16)
                    picked[m, j] = jnp.broadcast_to(
                        jnp.sum(chosen * weight[j : j + 1], axis=1, keepdims=True),
                        (capacity, 128),
                    )

        tables(ids, weights, experts, choose, picked)
        square = []
        for m in range(2):
            values = saved[0, m].astype(f32)
            square.append(jnp.sum(values * values, axis=1, keepdims=True))
        sq_send[...] = jnp.where(lane < 64, square[0], square[1])

        def pack(m, k, value):
            packed = dot(choose[m].reshape(experts * capacity, tok), value)
            packed = packed.reshape(experts, capacity, feat)
            if k == 1:
                packed = packed * picked[m][:, :, :1]
            packed = packed.astype(bf16)
            rows[m, k, 0] = packed[0]
            rows_out[m, k, 1:] = packed[1:]

        def pack_for(choose, picked, dst, value):
            low = far[0] if dst is rows_up else 1
            packed = dot(choose[1, low:].reshape((experts - low) * capacity, tok), value)
            packed = packed.reshape(experts - low, capacity, feat) * picked[1, low:][:, :, :1]
            dst[low:] = packed.astype(bf16)

        def pack_near(value):
            high = far[0]
            packed = dot(choose[1, :high].reshape(high * capacity, tok), value)
            packed = packed.reshape(high, capacity, feat) * picked[1, :high][:, :, :1]
            packed = packed.astype(bf16)
            rows[1, 1, 0] = packed[0]
            rows_out[1, 1, 1:high] = packed[1:]

        for load in loads:
            load.wait()
        neighbours = (s > 0).astype(jnp.int32) + (s < sections - 1).astype(jnp.int32)
        pl.semaphore_wait(barrier, len(greet) + experts * neighbours)

        start(squares_copy())
        for i in range(3):
            start(weight_copy(i))
        if line:

            @pl.when(inner == 1)
            def _():
                for i in range(2):
                    routes(i).start()

        @pl.when(s < sections - 1)
        def _():
            for i in range(2):
                routes_up(i).start()

        @pl.when(s == sections - 1)
        def _():
            sec_recv[...] = loss_grad[...]
            for i in range(2):
                routes_top(i).start()

        pack(0, 1, cot_in[0])
        send_rows(0, 1)
        if line:

            @pl.when(inner == 1)
            def _():
                for i in range(2):
                    routes(i).wait_recv()
                tables(ids_far, weights_far, 2, choose_far, picked_far)

        @pl.when(s > 0)
        def _():
            for i in range(2):
                routes_up(i).wait_recv()
            tables(ids_up, weights_up, experts, choose_up, picked_up, (1,))

        @pl.when(s == sections - 2)
        def _():
            for i in range(2):
                routes_top(i).wait_recv()
            tables(ids_top, weights_top, experts, choose_top, picked_top, (1,))

        squares_copy().wait_recv()
        total = sq_send[...] + sq_recv[...]
        roots = [
            jnp.sqrt(total[:, 64 * m : 64 * m + 1] / model + epsilon) for m in range(2)
        ]

        def normed_of(m):
            return saved[0, m].astype(f32) / roots[m]

        for m in range(2):
            xin[m] = (normed_of(m) * gain[...]).astype(bf16)
            pack(m, 0, xin[m])
            if m == 0:
                send_rows(0, 0)

        for i in range(3):
            weight_copy(i).wait_recv()

        def relay(m, k):
            if not relayed[m][k]:
                return

            @pl.when(inner == 1)
            def _():
                whole(m, k).wait_recv()
                packed = dot(choose_far[m].reshape(2 * capacity, tok), full_recv[m, k])
                packed = packed.reshape(2, capacity, feat)
                if k == 1:
                    packed = packed * picked_far[m][:, :, :1]
                packed = packed.astype(bf16)
                rows_out[m, k, 2] = packed[1]
                passed_on(m, k).start()
                rows[m, k, 2] = packed[0]

        def receive(m, k, j):
            if relayed[m][k] and j == 2:

                @pl.when(inner == 0)
                def _():
                    arrival(m, k, j).wait_recv()

            else:
                arrival(m, k, j).wait_recv()

        def consume(m, k, i):
            lo, n = chunks[i]
            for j in range(max(1, lo), lo + n):
                receive(m, k, j)
            flat = rows[m, k, lo : lo + n].reshape(n * capacity, feat)
            if k == 0:
                done = dot(flat, wgu[...]).reshape(n, capacity, 4 * hid)
                part_gu[m, lo : lo + n] = done
                gu_send[m, lo : lo + n] = done.astype(bf16)
            else:
                done = contract_last(flat, wd[...]).reshape(n, capacity, 2 * hid)
                part_h[m, lo : lo + n] = done
                h_send[m, lo : lo + n] = done.astype(bf16)
            exchange(m, k, i).start()

        def prepare(m, i):
            lo, n = chunks[i]
            exchange(m, 0, i).wait_recv()
            for j in range(lo, lo + n):
                both = part_gu[m, j] + gu_recv[m, j].astype(f32)
                gate, up = both[:, : 2 * hid], both[:, 2 * hid :]
                sigma = jax.nn.sigmoid(gate)
                for_up = gate * sigma
                for_gate = up * (sigma * (1.0 + gate * (1.0 - sigma)))
                part_gu[m, j, :, : 2 * hid] = for_gate
                part_gu[m, j, :, 2 * hid :] = for_up
                part_in[m, j] = for_gate * gate + for_up * up

        def produce(m, *group):
            for i in group:
                exchange(m, 1, i).wait_recv()
            ones = jnp.ones((8, 2 * hid), bf16)
            first, count = chunks[min(group)][0], sum(chunks[i][1] for i in group)
            for j in range(first, first + count):
                hidden = part_h[m, j] + h_recv[m, j].astype(f32)
                for a in (0, 2 * hid):
                    grads[m, j, :, a : a + 2 * hid] = (
                        hidden * part_gu[m, j, :, a : a + 2 * hid]
                    ).astype(bf16)
                scalars = contract_last(ones, (hidden * part_in[m, j]).astype(bf16))
                if j == 0:
                    sc_recv[m, j, :, :capacity] = scalars
                else:
                    sc_send[m, j, :, :capacity] = scalars
                    start(give_scalars(m, j))
            flat = grads[m, first : first + count].reshape(count * capacity, 4 * hid)
            done = contract_last(flat, wgu[...]).reshape(count, capacity, feat).astype(bf16)
            for j in range(first, first + count)[::-1]:
                if j == 0:
                    ret_recv[m, 0] = done[0]
                else:
                    ret_send[m, j] = done[j - first]
                    start(give_back(m, j))

        def combine(m, incoming):
            for j in js[1:]:
                given_scalars(m, j).wait_recv()
            inner = jnp.zeros((tok, 8), f32)
            for j in js:
                inner = inner + lax.dot_general(
                    choose[m, j], sc_recv[m, j, :, :capacity].astype(bf16),
                    (((0,), (1,)), ((), ())), preferred_element_type=f32,
                )
            inner = inner[:, :1]
            for j in js[1:]:
                given_back(m, j).wait_recv()
            cot = contract_first(
                choose[m].reshape(experts * capacity, tok),
                ret_recv[m].reshape(experts * capacity, feat),
            )
            scaled = gain[...] * cot
            normed = normed_of(m)
            out[0, m] = (
                incoming + (scaled - normed * (inner / model)) / roots[m]
            ).astype(bf16)

        last = len(chunks)
        consume(0, 1, 0)
        consume(0, 0, 0)
        relay(0, 1)
        consume(0, 1, 1)
        consume(0, 0, 1)
        for i in range(2, last):
            consume(0, 1, i)
        for i in range(2, last):
            consume(0, 0, i)
        send_rows(1, 0)
        @pl.when(s == sections - 2)
        def _():
            pack_for(choose_top, picked_top, rows_top, loss_grad[...])
            for j in js[1:]:
                ascend(j).start()

        prepare(0, 0)
        produce(0, 0)
        prepare(0, 1)
        produce(0, 1)
        prepare(0, 2)
        produce(0, 2)
        relay(1, 0)
        prepare(0, 3)
        produce(0, 3)
        for i in range(last):
            consume(1, 0, i)

        @pl.when(s > 0)
        def _():
            combine(0, cot_in[0].astype(f32))
            section_copy().start()
            pack_for(choose_up, picked_up, rows_up, out[0, 0])
            for j in far:
                descend(j).start()

        @pl.when(s < sections - 1)
        def _():
            section_copy().wait_recv()
            pack_near(sec_recv[...])
            for j in near:
                direct(1, 1, j).start()

        @pl.when(s == sections - 1)
        def _():
            pack_near(sec_recv[...])

        consume(1, 1, 0)
        consume(1, 1, 2)
        consume(1, 1, 3)
        consume(1, 1, 1)
        prepare(1, 2)
        prepare(1, 3)
        prepare(1, 0)
        prepare(1, 1)
        produce(1, 2, 3)
        produce(1, 0, 1)

        @pl.when(s == 0)
        def _():
            combine(0, cot_in[0].astype(f32))

        combine(1, sec_recv[...].astype(f32))

        for copy in started:
            copy.wait_send()
        for m in range(2):
            for k in range(2):
                for i in range(last):
                    exchange(m, k, i).wait_send()
                if m == 1 and k == 1:

                    @pl.when(s < sections - 1)
                    def _():
                        for j in near:
                            direct(1, 1, j).wait_send()

                    continue
                if not relayed[m][k]:
                    for j in js[1:]:
                        direct(m, k, j).wait_send()
                    continue
                direct(m, k, 1).wait_send()
                direct(m, k, 2).wait_send()

                @pl.when(inner == 1)
                def _():
                    whole(m, k).wait_send()

                @pl.when(inner == 0)
                def _():
                    direct(m, k, 3).wait_send()

        if line:

            @pl.when(inner == 1)
            def _():
                for i in range(2):
                    routes(i).wait_send()

        @pl.when(s > 0)
        def _():
            section_copy().wait_send()
            for j in far:
                descend(j).wait_send()

        @pl.when(s == sections - 2)
        def _():
            for j in js[1:]:
                ascend(j).wait_send()

        @pl.when(s == sections - 1)
        def _():
            for i in range(2):
                routes_top(i).wait_send()

        @pl.when(s < sections - 1)
        def _():
            for i in range(2):
                routes_up(i).wait_send()

    return kernel


def solution(mesh):
    sections, tensors = mesh.shape["section"], mesh.shape["tensor"]
    experts = mesh.shape["expert"] // 2

    def local(saved, cot_in, loss_grad, ids, weights, gain, wg, wu, wd):
        tok, feat = saved.shape[2], saved.shape[3]
        hid = wg.shape[3]
        named = 3 * tok * ids.shape[3] // (2 * experts)
        cap = -(-named // 16) * 16
        vmem = pl.BlockSpec(memory_space=pltpu.VMEM)
        hbm = pl.BlockSpec(memory_space=pl.ANY)
        dma = pltpu.SemaphoreType.DMA
        scratch = [
            pltpu.VMEM((feat, 4 * hid), bf16), pltpu.VMEM((2 * hid, feat), bf16), dma((3,)),
            pltpu.VMEM((2, experts, cap, tok), bf16), pltpu.VMEM((2, experts, cap, 128), f32),
            pltpu.VMEM((2, 2, experts, cap, feat), bf16),
            pltpu.VMEM((2, 2, experts, cap, feat), bf16),
            pltpu.VMEM((2, experts, cap, 4 * hid), f32),
            pltpu.VMEM((2, experts, cap, 2 * hid), f32),
            pltpu.VMEM((2, experts, cap, 2 * hid), f32),
            pltpu.VMEM((2, experts, cap, 4 * hid), bf16),
            pltpu.VMEM((2, experts, cap, 4 * hid), bf16),
            pltpu.VMEM((2, experts, cap, 2 * hid), bf16),
            pltpu.VMEM((2, experts, cap, 2 * hid), bf16),
            pltpu.VMEM((2, experts, cap, 4 * hid), bf16),
            pltpu.VMEM((2, experts, cap, feat), bf16),
            pltpu.VMEM((2, experts, cap, feat), bf16),
            pltpu.VMEM((2, experts, 8, 128), f32), pltpu.VMEM((2, experts, 8, 128), f32),
            pltpu.VMEM((tok, 128), f32), pltpu.VMEM((tok, 128), f32),
            pltpu.VMEM((tok, feat), bf16),
            pltpu.VMEM((2, tok, feat), bf16), pltpu.VMEM((2, 2, tok, feat), bf16),
            pltpu.VMEM((1, 2, ids.shape[3], tok), jnp.int32),
            pltpu.VMEM((1, 2, ids.shape[3], tok), f32),
            pltpu.VMEM((2, 2, cap, tok), bf16), pltpu.VMEM((2, 2, cap, 128), f32),
            pltpu.VMEM((experts, cap, feat), bf16),
            pltpu.VMEM((1, 2, ids.shape[3], tok), jnp.int32),
            pltpu.VMEM((1, 2, ids.shape[3], tok), f32),
            pltpu.VMEM((2, experts, cap, tok), bf16), pltpu.VMEM((2, experts, cap, 128), f32),
        ]
        scratch += scratch[-5:]
        pair = [dma, dma]
        scratch += [dma((3,))] * 2 + [dma((2, 2, experts))] * 2 + [dma((2, 2, min(experts, 4)))] * 2
        scratch += [dma((2, experts))] * 4 + pair + pair + [dma((2, 2))] * 2 + [dma((2,))] * 2
        scratch += ([dma((experts,))] + [dma((2,))] * 2) * 2
        return pl.pallas_call(
            make_kernel(sections, tensors, experts, cap),
            out_shape=jax.ShapeDtypeStruct((1, 2, tok, feat), bf16),
            in_specs=[vmem] * 6 + [hbm] * 3,
            out_specs=vmem,
            scratch_shapes=scratch,
            compiler_params=pltpu.CompilerParams(
                collective_id=0, has_side_effects=True, vmem_limit_bytes=62 * 1024 * 1024
            ),
            name="expert_back",
        )(
            saved, cot_in, loss_grad, ids.transpose(0, 1, 3, 2), weights.transpose(0, 1, 3, 2),
            gain, wg, wu, wd,
        )

    in_specs = (
        P("section", None, "expert", "tensor"),
        P("section", "expert", "tensor"),
        P("expert", "tensor"),
        P("section", None, "expert", None),
        P("section", None, "expert", None),
        P("section", "tensor"),
        P("section", "expert", "tensor", None),
        P("section", "expert", "tensor", None),
        P("section", "expert", None, "tensor"),
    )
    out_specs = P("section", None, "expert", "tensor")
    return jax.shard_map(local, mesh=mesh, in_specs=in_specs, out_specs=out_specs, check_vma=False)
```

```python
import jax
import jax.numpy as jnp
from jax import lax
from jax.experimental import pallas as pl
from jax.experimental.pallas import tpu as pltpu
from jax.sharding import PartitionSpec as P

epsilon = 1e-06
MESH = pl.DeviceIdType.MESH
bf16 = jnp.bfloat16
f32 = jnp.float32


def contract_last(left, right):
    return lax.dot_general(left, right, (((1,), (1,)), ((), ())), preferred_element_type=f32)


def contract_first(left, right):
    return lax.dot_general(left, right, (((0,), (0,)), ((), ())), preferred_element_type=f32)


def dot(left, right):
    return jnp.dot(left, right, preferred_element_type=f32)


def make_kernel(sections, tensors, experts, capacity):

    def kernel(
        saved, cot_in, loss_grad, ids, weights, gain, wg_hbm, wu_hbm, wd_hbm, out,
        wgu, wd, w_sem, choose, picked, rows_out, rows, part_gu, part_h, part_in,
        gu_send, gu_recv, h_send, h_recv, grads, ret_send, ret_recv,
        sc_send, sc_recv, sq_send, sq_recv, sec_recv,
        xin, full_recv, ids_far, weights_far, choose_far, picked_far,
        rows_up, ids_up, weights_up, choose_up, picked_up,
        rows_top, ids_top, weights_top, choose_top, picked_top,
        w_s, w_r, d_s, d_r, y_s, y_r, r_s, r_r, v_s, v_r, q_s, q_r, c_s, c_r,
        f_s, f_r, i_s, i_r, u_s, g_s, g_r, t_s, h_s, h_r,
    ):
        s = lax.axis_index("section")
        t = lax.axis_index("tensor")
        x = lax.axis_index("expert")
        e, q = x // 2, x % 2
        tok = saved.shape[2]
        feat = saved.shape[3]
        top = ids.shape[2]
        hid = wd_hbm.shape[2]
        model = feat * tensors
        js = list(range(experts))

        loads = [
            pltpu.make_async_copy(wd_hbm.at[0, 0], wd.at[0:hid], w_sem.at[0]),
            pltpu.make_async_copy(wg_hbm.at[0, 0], wgu.at[:, 0:hid], w_sem.at[1]),
            pltpu.make_async_copy(wu_hbm.at[0, 0], wgu.at[:, 2 * hid : 3 * hid], w_sem.at[2]),
        ]
        for load in loads:
            load.start()

        line = experts == 4
        relayed = ((False, True), (True, False)) if line else ((False, False), (False, False))
        side = e // 2
        inner = ((e + 1) // 2) % 2
        far_slot = 3 - inner

        def expert_at(j):
            if line and j >= 2:
                return 2 - side if j == 2 else 3 * (1 - side)
            other, bit = e, 1
            while bit < experts:
                if j & bit:
                    other = other + bit - 2 * bit * ((e // bit) % 2)
                bit *= 2
            return other

        lane_peer = lambda j: (s, t, 2 * expert_at(j) + q)
        partner = (s, t, 2 * e + 1 - q)
        y_peer = (s, 1 - t, x)

        barrier = pltpu.get_barrier_semaphore()
        greet = [lane_peer(j) for j in js[1:]] + [partner, y_peer]
        for device in greet:
            pl.semaphore_signal(barrier, inc=1, device_id=device, device_id_type=MESH)

        @pl.when(s > 0)
        def _():
            for j in js:
                below = (s - 1, t, 2 * expert_at(j) + q)
                pl.semaphore_signal(barrier, inc=1, device_id=below, device_id_type=MESH)

        @pl.when(s < sections - 1)
        def _():
            for j in js:
                above = (s + 1, t, 2 * expert_at(j) + q)
                pl.semaphore_signal(barrier, inc=1, device_id=above, device_id_type=MESH)

        def remote(src, dst, send, recv, device):
            return pltpu.make_async_remote_copy(
                src_ref=src, dst_ref=dst, send_sem=send, recv_sem=recv,
                device_id=device, device_id_type=MESH,
            )

        def weight_copy(i):
            ref = (
                (wd.at[0:hid], wd.at[hid : 2 * hid]),
                (wgu.at[:, 0:hid], wgu.at[:, hid : 2 * hid]),
                (wgu.at[:, 2 * hid : 3 * hid], wgu.at[:, 3 * hid : 4 * hid]),
            )[i]
            return remote(ref[0], ref[1], w_s.at[i], w_r.at[i], partner)

        def landing(j):
            return far_slot if line and j >= 2 else j

        def direct(m, k, j):
            return remote(
                rows_out.at[m, k, j], rows.at[m, k, landing(j)],
                d_s.at[m, k, j], d_r.at[m, k, landing(j)], lane_peer(j),
            )

        def passed_on(m, k):
            return remote(
                rows_out.at[m, k, 2], rows.at[m, k, 2], d_s.at[m, k, 2], d_r.at[m, k, 2],
                lane_peer(1),
            )

        def arrival(m, k, j):
            return remote(
                rows_out.at[m, k, j], rows.at[m, k, j], d_s.at[m, k, j], d_r.at[m, k, j],
                lane_peer(j),
            )

        def whole(m, k):
            src = xin.at[m] if k == 0 else (cot_in.at[0], sec_recv)[m]
            return remote(src, full_recv.at[m, k], f_s.at[m, k], f_r.at[m, k], lane_peer(2))

        def routes(i):
            src, dst = ((ids, ids_far), (weights, weights_far))[i]
            return remote(src, dst, i_s.at[i], i_r.at[i], lane_peer(2))

        def send_rows(m, k):
            if not relayed[m][k]:
                for j in js[1:] if line else order:
                    direct(m, k, j).start()
                return

            @pl.when(inner == 1)
            def _():
                whole(m, k).start()
                direct(m, k, 1).start()

            @pl.when(inner == 0)
            def _():
                for j in (1, 2, 3):
                    direct(m, k, j).start()

        def exchange(m, k, i):
            lo, n = chunks[i]
            src, dst = ((gu_send, gu_recv), (h_send, h_recv))[k]
            return remote(
                src.at[m, lo : lo + n], dst.at[m, lo : lo + n], y_s.at[m, k, i], y_r.at[m, k, i],
                y_peer,
            )

        def give_back(m, j):
            return remote(
                ret_send.at[m, j], ret_recv.at[m, landing(j)], r_s.at[m, j],
                r_r.at[m, landing(j)], lane_peer(j),
            )

        def given_back(m, j):
            return remote(
                ret_send.at[m, j], ret_recv.at[m, j], r_s.at[m, j], r_r.at[m, j], lane_peer(j)
            )

        def give_scalars(m, j):
            return remote(
                sc_send.at[m, j], sc_recv.at[m, landing(j)], v_s.at[m, j],
                v_r.at[m, landing(j)], lane_peer(j),
            )

        def given_scalars(m, j):
            return remote(
                sc_send.at[m, j], sc_recv.at[m, j], v_s.at[m, j], v_r.at[m, j], lane_peer(j)
            )

        def squares_copy():
            return remote(sq_send, sq_recv, q_s, q_r, y_peer)

        def section_copy():
            return remote(out.at[0, 0], sec_recv, c_s, c_r, (s - 1, t, x))

        def descend(j):
            return remote(
                rows_up.at[j], rows.at[1, 1, landing(j)], u_s.at[j], d_r.at[1, 1, landing(j)],
                (s - 1, t, 2 * expert_at(j) + q),
            )

        def ascend(j):
            return remote(
                rows_top.at[j], rows.at[1, 1, landing(j)], t_s.at[j], d_r.at[1, 1, landing(j)],
                (s + 1, t, 2 * expert_at(j) + q),
            )

        def routes_top(i):
            src, dst = ((ids, ids_top), (weights, weights_top))[i]
            return remote(src, dst, h_s.at[i], h_r.at[i], (s - 1, t, x))

        def routes_up(i):
            src, dst = ((ids, ids_up), (weights, weights_up))[i]
            return remote(src, dst, g_s.at[i], g_r.at[i], (s + 1, t, x))

        started = []

        def start(copy):
            copy.start()
            started.append(copy)

        quarter = max(1, experts // 4)
        near, far = js[1 : 2 * quarter], js[2 * quarter :]
        chunks = [(i * quarter, quarter) for i in range(experts // quarter)]
        order = js[3 * quarter :] + js[1 : 2 * quarter] + js[2 * quarter : 3 * quarter]

        lane = lax.broadcasted_iota(jnp.int32, (tok, 128), 1)
        later = (
            lax.broadcasted_iota(jnp.int32, (tok, tok), 0)
            < lax.broadcasted_iota(jnp.int32, (tok, tok), 1)
        ).astype(f32).astype(bf16)
        slot = lax.broadcasted_iota(jnp.int32, (capacity, tok), 0).astype(f32)

        def tables(ids, weights, count, choose, picked, batches=(0, 1)):
            height = max(8, count)
            row = lax.broadcasted_iota(jnp.int32, (height, tok), 0)
            named = jnp.full((height, tok), experts, jnp.int32)
            for j in range(count):
                named = jnp.where(row == j, expert_at(j), named)
            for m in batches:
                hit = jnp.zeros((height, tok), f32)
                weight = jnp.zeros((height, tok), f32)
                for k in range(top):
                    same = (ids[0, m, k : k + 1, :] == named).astype(f32)
                    hit = hit + same
                    weight = weight + same * weights[0, m, k : k + 1, :]
                position = dot(hit.astype(bf16), later)
                for j in range(count):
                    chosen = (position[j : j + 1] == slot).astype(f32) * hit[j : j + 1]
                    choose[m, j] = chosen.astype(bf16)
                    picked[m, j] = jnp.broadcast_to(
                        jnp.sum(chosen * weight[j : j + 1], axis=1, keepdims=True),
                        (capacity, 128),
                    )

        tables(ids, weights, experts, choose, picked, (0,))
        square = []
        for m in range(2):
            values = saved[0, m].astype(f32)
            square.append(jnp.sum(values * values, axis=1, keepdims=True))
        sq_send[...] = jnp.where(lane < 64, square[0], square[1])

        def pack(m, k, value):
            packed = dot(choose[m].reshape(experts * capacity, tok), value)
            packed = packed.reshape(experts, capacity, feat)
            if k == 1:
                packed = packed * picked[m][:, :, :1]
            packed = packed.astype(bf16)
            rows[m, k, 0] = packed[0]
            rows_out[m, k, 1:] = packed[1:]

        def pack_for(choose, picked, dst, value):
            low = far[0] if dst is rows_up else 1
            packed = dot(choose[1, low:].reshape((experts - low) * capacity, tok), value)
            packed = packed.reshape(experts - low, capacity, feat) * picked[1, low:][:, :, :1]
            dst[low:] = packed.astype(bf16)

        def pack_near(value):
            high = far[0]
            packed = dot(choose[1, :high].reshape(high * capacity, tok), value)
            packed = packed.reshape(high, capacity, feat) * picked[1, :high][:, :, :1]
            packed = packed.astype(bf16)
            rows[1, 1, 0] = packed[0]
            rows_out[1, 1, 1:high] = packed[1:]

        for load in loads:
            load.wait()
        neighbours = (s > 0).astype(jnp.int32) + (s < sections - 1).astype(jnp.int32)
        pl.semaphore_wait(barrier, len(greet) + experts * neighbours)

        start(squares_copy())
        for i in range(3):
            start(weight_copy(i))
        if line:

            @pl.when(inner == 1)
            def _():
                for i in range(2):
                    routes(i).start()

        @pl.when(s < sections - 1)
        def _():
            for i in range(2):
                routes_up(i).start()

        @pl.when(s == sections - 1)
        def _():
            sec_recv[...] = loss_grad[...]
            for i in range(2):
                routes_top(i).start()

        pack(0, 1, cot_in[0])
        send_rows(0, 1)
        tables(ids, weights, experts, choose, picked, (1,))
        if line:

            @pl.when(inner == 1)
            def _():
                for i in range(2):
                    routes(i).wait_recv()
                tables(ids_far, weights_far, 2, choose_far, picked_far)

        @pl.when(s > 0)
        def _():
            for i in range(2):
                routes_up(i).wait_recv()
            tables(ids_up, weights_up, experts, choose_up, picked_up, (1,))

        @pl.when(s == sections - 2)
        def _():
            for i in range(2):
                routes_top(i).wait_recv()
            tables(ids_top, weights_top, experts, choose_top, picked_top, (1,))

        squares_copy().wait_recv()
        total = sq_send[...] + sq_recv[...]
        roots = [
            jnp.sqrt(total[:, 64 * m : 64 * m + 1] / model + epsilon) for m in range(2)
        ]

        def normed_of(m):
            return saved[0, m].astype(f32) / roots[m]

        for m in range(2):
            xin[m] = (normed_of(m) * gain[...]).astype(bf16)
            pack(m, 0, xin[m])
            if m == 0:
                send_rows(0, 0)

        for i in range(3):
            weight_copy(i).wait_recv()

        def relay(m, k):
            if not relayed[m][k]:
                return

            @pl.when(inner == 1)
            def _():
                whole(m, k).wait_recv()
                packed = dot(choose_far[m].reshape(2 * capacity, tok), full_recv[m, k])
                packed = packed.reshape(2, capacity, feat)
                if k == 1:
                    packed = packed * picked_far[m][:, :, :1]
                packed = packed.astype(bf16)
                rows_out[m, k, 2] = packed[1]
                passed_on(m, k).start()
                rows[m, k, 2] = packed[0]

        def receive(m, k, j):
            if relayed[m][k] and j == 2:

                @pl.when(inner == 0)
                def _():
                    arrival(m, k, j).wait_recv()

            else:
                arrival(m, k, j).wait_recv()

        def consume(m, k, i):
            lo, n = chunks[i]
            for j in range(max(1, lo), lo + n):
                receive(m, k, j)
            flat = rows[m, k, lo : lo + n].reshape(n * capacity, feat)
            if k == 0:
                done = dot(flat, wgu[...]).reshape(n, capacity, 4 * hid)
                part_gu[m, lo : lo + n] = done
                gu_send[m, lo : lo + n] = done.astype(bf16)
            else:
                done = contract_last(flat, wd[...]).reshape(n, capacity, 2 * hid)
                part_h[m, lo : lo + n] = done
                h_send[m, lo : lo + n] = done.astype(bf16)
            exchange(m, k, i).start()

        def prepare(m, i):
            lo, n = chunks[i]
            exchange(m, 0, i).wait_recv()
            for j in range(lo, lo + n):
                both = part_gu[m, j] + gu_recv[m, j].astype(f32)
                gate, up = both[:, : 2 * hid], both[:, 2 * hid :]
                sigma = jax.nn.sigmoid(gate)
                for_up = gate * sigma
                for_gate = up * (sigma * (1.0 + gate * (1.0 - sigma)))
                part_gu[m, j, :, : 2 * hid] = for_gate
                part_gu[m, j, :, 2 * hid :] = for_up
                part_in[m, j] = for_gate * gate + for_up * up

        def produce(m, *group):
            for i in group:
                exchange(m, 1, i).wait_recv()
            ones = jnp.ones((8, 2 * hid), bf16)
            first, count = chunks[min(group)][0], sum(chunks[i][1] for i in group)
            for j in range(first, first + count):
                hidden = part_h[m, j] + h_recv[m, j].astype(f32)
                for a in (0, 2 * hid):
                    grads[m, j, :, a : a + 2 * hid] = (
                        hidden * part_gu[m, j, :, a : a + 2 * hid]
                    ).astype(bf16)
                scalars = contract_last(ones, (hidden * part_in[m, j]).astype(bf16))
                if j == 0:
                    sc_recv[m, j, :, :capacity] = scalars
                else:
                    sc_send[m, j, :, :capacity] = scalars
                    start(give_scalars(m, j))
            flat = grads[m, first : first + count].reshape(count * capacity, 4 * hid)
            done = contract_last(flat, wgu[...]).reshape(count, capacity, feat).astype(bf16)
            for j in range(first, first + count)[::-1]:
                if j == 0:
                    ret_recv[m, 0] = done[0]
                else:
                    ret_send[m, j] = done[j - first]
                    start(give_back(m, j))

        def combine(m, incoming):
            for j in js[1:]:
                given_scalars(m, j).wait_recv()
            inner = jnp.zeros((tok, 8), f32)
            for j in js:
                inner = inner + lax.dot_general(
                    choose[m, j], sc_recv[m, j, :, :capacity].astype(bf16),
                    (((0,), (1,)), ((), ())), preferred_element_type=f32,
                )
            inner = inner[:, :1]
            for j in js[1:]:
                given_back(m, j).wait_recv()
            cot = contract_first(
                choose[m].reshape(experts * capacity, tok),
                ret_recv[m].reshape(experts * capacity, feat),
            )
            scaled = gain[...] * cot
            normed = normed_of(m)
            out[0, m] = (
                incoming + (scaled - normed * (inner / model)) / roots[m]
            ).astype(bf16)

        last = len(chunks)
        consume(0, 1, 0)
        consume(0, 0, 0)
        relay(0, 1)
        consume(0, 1, 1)
        consume(0, 0, 1)
        for i in range(2, last):
            consume(0, 1, i)
        send_rows(1, 0)
        for i in range(2, last):
            consume(0, 0, i)
        @pl.when(s == sections - 2)
        def _():
            pack_for(choose_top, picked_top, rows_top, loss_grad[...])
            for j in js[1:]:
                ascend(j).start()

        prepare(0, 0)
        produce(0, 0)
        prepare(0, 1)
        produce(0, 1)
        prepare(0, 2)
        produce(0, 2)
        relay(1, 0)
        prepare(0, 3)
        produce(0, 3)
        for i in range(last):
            consume(1, 0, i)

        @pl.when(s > 0)
        def _():
            combine(0, cot_in[0].astype(f32))
            section_copy().start()
            pack_for(choose_up, picked_up, rows_up, out[0, 0])
            for j in far:
                descend(j).start()

        @pl.when(s < sections - 1)
        def _():
            section_copy().wait_recv()
            pack_near(sec_recv[...])
            for j in near:
                direct(1, 1, j).start()

        @pl.when(s == sections - 1)
        def _():
            pack_near(sec_recv[...])

        consume(1, 1, 0)
        consume(1, 1, 2)
        consume(1, 1, 3)
        consume(1, 1, 1)
        prepare(1, 2)
        prepare(1, 3)
        prepare(1, 0)
        prepare(1, 1)
        produce(1, 2, 3)
        produce(1, 0, 1)

        @pl.when(s == 0)
        def _():
            combine(0, cot_in[0].astype(f32))

        combine(1, sec_recv[...].astype(f32))

        for copy in started:
            copy.wait_send()
        for m in range(2):
            for k in range(2):
                for i in range(last):
                    exchange(m, k, i).wait_send()
                if m == 1 and k == 1:

                    @pl.when(s < sections - 1)
                    def _():
                        for j in near:
                            direct(1, 1, j).wait_send()

                    continue
                if not relayed[m][k]:
                    for j in js[1:]:
                        direct(m, k, j).wait_send()
                    continue
                direct(m, k, 1).wait_send()
                direct(m, k, 2).wait_send()

                @pl.when(inner == 1)
                def _():
                    whole(m, k).wait_send()

                @pl.when(inner == 0)
                def _():
                    direct(m, k, 3).wait_send()

        if line:

            @pl.when(inner == 1)
            def _():
                for i in range(2):
                    routes(i).wait_send()

        @pl.when(s > 0)
        def _():
            section_copy().wait_send()
            for j in far:
                descend(j).wait_send()

        @pl.when(s == sections - 2)
        def _():
            for j in js[1:]:
                ascend(j).wait_send()

        @pl.when(s == sections - 1)
        def _():
            for i in range(2):
                routes_top(i).wait_send()

        @pl.when(s < sections - 1)
        def _():
            for i in range(2):
                routes_up(i).wait_send()

    return kernel


def solution(mesh):
    sections, tensors = mesh.shape["section"], mesh.shape["tensor"]
    experts = mesh.shape["expert"] // 2

    def local(saved, cot_in, loss_grad, ids, weights, gain, wg, wu, wd):
        tok, feat = saved.shape[2], saved.shape[3]
        hid = wg.shape[3]
        named = 3 * tok * ids.shape[3] // (2 * experts)
        cap = -(-named // 16) * 16
        vmem = pl.BlockSpec(memory_space=pltpu.VMEM)
        hbm = pl.BlockSpec(memory_space=pl.ANY)
        dma = pltpu.SemaphoreType.DMA
        scratch = [
            pltpu.VMEM((feat, 4 * hid), bf16), pltpu.VMEM((2 * hid, feat), bf16), dma((3,)),
            pltpu.VMEM((2, experts, cap, tok), bf16), pltpu.VMEM((2, experts, cap, 128), f32),
            pltpu.VMEM((2, 2, experts, cap, feat), bf16),
            pltpu.VMEM((2, 2, experts, cap, feat), bf16),
            pltpu.VMEM((2, experts, cap, 4 * hid), f32),
            pltpu.VMEM((2, experts, cap, 2 * hid), f32),
            pltpu.VMEM((2, experts, cap, 2 * hid), f32),
            pltpu.VMEM((2, experts, cap, 4 * hid), bf16),
            pltpu.VMEM((2, experts, cap, 4 * hid), bf16),
            pltpu.VMEM((2, experts, cap, 2 * hid), bf16),
            pltpu.VMEM((2, experts, cap, 2 * hid), bf16),
            pltpu.VMEM((2, experts, cap, 4 * hid), bf16),
            pltpu.VMEM((2, experts, cap, feat), bf16),
            pltpu.VMEM((2, experts, cap, feat), bf16),
            pltpu.VMEM((2, experts, 8, 128), f32), pltpu.VMEM((2, experts, 8, 128), f32),
            pltpu.VMEM((tok, 128), f32), pltpu.VMEM((tok, 128), f32),
            pltpu.VMEM((tok, feat), bf16),
            pltpu.VMEM((2, tok, feat), bf16), pltpu.VMEM((2, 2, tok, feat), bf16),
            pltpu.VMEM((1, 2, ids.shape[3], tok), jnp.int32),
            pltpu.VMEM((1, 2, ids.shape[3], tok), f32),
            pltpu.VMEM((2, 2, cap, tok), bf16), pltpu.VMEM((2, 2, cap, 128), f32),
            pltpu.VMEM((experts, cap, feat), bf16),
            pltpu.VMEM((1, 2, ids.shape[3], tok), jnp.int32),
            pltpu.VMEM((1, 2, ids.shape[3], tok), f32),
            pltpu.VMEM((2, experts, cap, tok), bf16), pltpu.VMEM((2, experts, cap, 128), f32),
        ]
        scratch += scratch[-5:]
        pair = [dma, dma]
        scratch += [dma((3,))] * 2 + [dma((2, 2, experts))] * 2 + [dma((2, 2, min(experts, 4)))] * 2
        scratch += [dma((2, experts))] * 4 + pair + pair + [dma((2, 2))] * 2 + [dma((2,))] * 2
        scratch += ([dma((experts,))] + [dma((2,))] * 2) * 2
        return pl.pallas_call(
            make_kernel(sections, tensors, experts, cap),
            out_shape=jax.ShapeDtypeStruct((1, 2, tok, feat), bf16),
            in_specs=[vmem] * 6 + [hbm] * 3,
            out_specs=vmem,
            scratch_shapes=scratch,
            compiler_params=pltpu.CompilerParams(
                collective_id=0, has_side_effects=True, vmem_limit_bytes=62 * 1024 * 1024
            ),
            name="expert_back",
        )(
            saved, cot_in, loss_grad, ids.transpose(0, 1, 3, 2), weights.transpose(0, 1, 3, 2),
            gain, wg, wu, wd,
        )

    in_specs = (
        P("section", None, "expert", "tensor"),
        P("section", "expert", "tensor"),
        P("expert", "tensor"),
        P("section", None, "expert", None),
        P("section", None, "expert", None),
        P("section", "tensor"),
        P("section", "expert", "tensor", None),
        P("section", "expert", "tensor", None),
        P("section", "expert", None, "tensor"),
    )
    out_specs = P("section", None, "expert", "tensor")
    return jax.shard_map(local, mesh=mesh, in_specs=in_specs, out_specs=out_specs, check_vma=False)
```
